32 devices in a mesh: section: 4 (over y, core), expert: 8 (over z, x).
Axes of the slice: x: 2, y: 2, z: 4, core: 2. Of those that a mesh axis runs over, the one named last changes fastest.
Arguments:
- activations: bfloat16 [4, 256, 4096], P('section', 'expert'), may hold values from -6 to 6
- norm_gain: float32 [4, 4096], P('section'), may hold values from 0.25 to 1.75
- in_proj: bfloat16 [4, 4096, 40960], P('section', None, 'expert'), may hold values from -0.09375 to 0.09375
- out_proj: bfloat16 [4, 40960, 4096], P('section', 'expert'), may hold values from -0.078125 to 0.078125
- expert_ids: int32 [4, 256, 1], P('section', 'expert'), may hold values from 0 to 7; in each aligned block of 32 rows (0 to 31, 32 to 63, ..., all dimensions but the last counted through in order) at most 8 rows name the same one
Outputs:
- passed: bfloat16 [4, 256, 4096], P('section', 'expert')
The draws below stay inside these ranges and needn't reach their ends.
Inputs may be any that keep to these rules, and one draw needn't show every extreme that they name: `expert_ids`: within the 32 rows of one device (aligned blocks of 32 rows along the token dimension of each layer), no expert is named by more than 8 rows.
All inputs are finite; a program needn't handle non-finite values.
Results may differ from the reference program's by a relative error of at most 0.0047.
Values may be sent and summed in bfloat16 or wider, within the bound.
A program may use at most 128 MiB of HBM per device.

```python
import math
import jax
import jax.numpy as jnp
import numpy as np
from jax import lax

D = 4096
FF_W = 5120
EXPERTS = 8
MB_TOK = 32
CAP = 8
TOKENS = 256
N_SECTION = 4
N_EXPERT = 8


def steps_of(stream_key, dims, split, smallest, largest):
    gain, own = 1.0, jax.random.fold_in(stream_key, 6)
    for dim, parts in split:
        steps = jnp.exp(jax.random.uniform(jax.random.fold_in(own, dim), (parts,), jnp.float32, smallest / len(split), largest / len(split)))
        gain = gain * jnp.repeat(steps, dims[dim] // parts).reshape([-1 if axis == dim else 1 for axis in range(len(dims))])
    return gain


def shared_out(own_key, own, number, rows, number_of, top, bound, lean):
    order = jax.random.permutation(own_key, number_of)
    heavy_load, common = portions_of(number_of, rows * top, bound, lean, True), portions_of(number_of, rows * top, bound, lean, False)
    places = jnp.arange(number_of)

    def named(lengths, turn):
        used = int((lengths > 0).sum())
        fixed = max(1, used // 4)
        shifted = fixed + (places - fixed + turn * (used - fixed)) % max(1, number_of - fixed)
        return jnp.zeros((number_of,), jnp.int32).at[order[jnp.where(places < fixed, places, shifted)]].set(jnp.asarray(lengths, jnp.int32))

    lengths = jnp.where(number % 4 == 0, named(heavy_load, number // 4), named(common, number - number // 4 - 1))
    mixed = jax.random.permutation(jax.random.fold_in(own, 3), number_of)
    source_of, sink = mixed[0:number_of // 2 * 2:2], mixed[1:number_of // 2 * 2:2]
    margin = jnp.minimum(lengths[source_of] - 1, bound - lengths[sink]) // 2
    margin = jnp.where((source_of == order[0]) | (sink == order[0]) | (lengths[sink] == 0), 0, jnp.maximum(margin, 0))
    shifted = jax.random.randint(jax.random.fold_in(own, 4), (number_of // 2,), 0, 1 << 20) % (margin + 1)
    lengths = lengths.at[source_of].add(-shifted).at[sink].add(shifted)
    members = jnp.searchsorted(jnp.cumsum(lengths), jnp.arange(rows * top), side="right").astype(jnp.int32)
    listing = members.reshape(top, rows).T
    listing = listing[jax.random.permutation(jax.random.fold_in(own, 1), rows)]
    turn = jax.random.randint(jax.random.fold_in(own, 2), (rows, 1), 0, top)
    return jnp.take_along_axis(listing, (jnp.arange(top)[None, :] + turn) % top, axis=1)


def portions_of(count, total, most, slope, full):
    portions = [(1 << 20) // math.isqrt(grade ** slope) + 1 for grade in range(1, count + 1)]
    largest = most if full else min(most, max(-(-total // count), total * portions[0] // sum(portions)))
    least = 1 if total - largest >= count - 1 else 0
    given, spare = [largest] + [least] * (count - 1), total - largest - least * (count - 1)
    while spare > 0:
        candidates = [i for i in range(1, count) if given[i] < largest] or [i for i in range(1, count) if given[i] < most]
        mass, remaining = sum([portions[i] for i in candidates]), spare
        for i in candidates:
            extra = min(most - given[i], max(1, remaining * portions[i] // mass), spare)
            given[i] = given[i] + extra
            spare = spare - extra
    return np.array(given)


def centred(key, shape, width, most, shards=(), kind=jnp.bfloat16):
    factor_of = steps_of(key, shape, shards, -0.22, 0.18) if shards else 1.0
    drawn = jax.random.normal(key, shape, jnp.float32) * width * factor_of
    return jnp.minimum(jnp.maximum(drawn, -most), most).astype(kind)


def setup_inputs(seed: int = 0) -> dict:
    key_list = jax.random.split(jax.random.key(seed), 6)
    activations = centred(key_list[0], (N_SECTION, TOKENS, D), 1.0, 6.0, ((0, 4), (1, 8)))
    norm_gain = jnp.clip(1.0 + 0.15 * jax.random.normal(key_list[1], (N_SECTION, D), jnp.float32), 0.25, 1.75)
    in_proj = centred(key_list[2], (N_SECTION, D, EXPERTS * FF_W), D ** -0.5, 0.09375, ((0, 4), (2, 8)))
    out_proj = centred(key_list[3], (N_SECTION, EXPERTS * FF_W, D), FF_W ** -0.5, 0.078125, ((0, 4), (1, 8)))
    expert_ids_keys = jax.random.split(jax.random.fold_in(key_list[4], 1), N_SECTION * TOKENS // MB_TOK)
    expert_ids_turns = jax.random.permutation(jax.random.fold_in(key_list[4], 3), N_SECTION * TOKENS // MB_TOK)
    expert_ids = jax.vmap(lambda own, number: shared_out(jax.random.fold_in(key_list[4], 2), own, number, MB_TOK, EXPERTS, 1, CAP, 2))(expert_ids_keys, expert_ids_turns).reshape((N_SECTION, TOKENS, 1))
    return {"activations": activations, "norm_gain": norm_gain, "in_proj": in_proj, "out_proj": out_proj, "expert_ids": expert_ids}


epsilon = 1e-06

def reference(activations, norm_gain, in_proj, out_proj, expert_ids):
    groups = N_EXPERT // EXPERTS
    slice_width = FF_W // groups
    results = []
    for section_index in range(N_SECTION):
        floats = activations[section_index].astype(jnp.float32)
        scale = lax.rsqrt(lax.optimization_barrier(jnp.mean(floats * floats, axis=-1, keepdims=True)) + epsilon)
        normed = (floats * scale * norm_gain[section_index][None, :]).astype(jnp.bfloat16)
        routed = expert_ids[section_index, :, 0].astype(jnp.int32)
        onehot = (routed[:, None] == jnp.arange(EXPERTS, dtype=jnp.int32)[None, :]).astype(jnp.int32)
        blocked = onehot.reshape(N_EXPERT, MB_TOK, EXPERTS)
        before = (jnp.cumsum(blocked, axis=1) - blocked).reshape(TOKENS, EXPERTS)
        ranks = lax.optimization_barrier(jnp.sum(before * onehot, axis=1)).astype(jnp.int32)
        slots = (jnp.arange(TOKENS, dtype=jnp.int32) // MB_TOK * CAP + ranks).astype(jnp.int32)
        buffer = jnp.zeros((EXPERTS, N_EXPERT * CAP, D), jnp.bfloat16).at[routed, slots].set(normed)
        first_proj = in_proj[section_index].reshape(D, EXPERTS, FF_W).transpose(1, 0, 2)
        second_proj = out_proj[section_index].reshape(EXPERTS, FF_W, D)

        def expert(operands):
            inputs, first, second = operands
            preact = jnp.dot(inputs, first, preferred_element_type=jnp.float32)
            hidden = jax.nn.gelu(preact, approximate=True).astype(jnp.bfloat16)
            summed = jnp.zeros((inputs.shape[0], D), jnp.float32)
            for shard in range(groups):
                piece = jnp.dot(hidden[:, shard * slice_width:(shard + 1) * slice_width], second[shard * slice_width:(shard + 1) * slice_width], preferred_element_type=jnp.float32)
                summed = summed + piece
            return summed
        outputs = lax.map(expert, (buffer, first_proj, second_proj))
        mixed_rows = outputs[routed, slots]
        results.append((floats + mixed_rows).astype(jnp.bfloat16))
    return jnp.roll(jnp.stack(results), 1, axis=0)
```

```python
import functools
import math

import jax
import jax.numpy as jnp
from jax import lax
from jax.experimental import pallas as pl
from jax.experimental.pallas import tpu as pltpu
from jax.sharding import PartitionSpec as P

EXPERTS = 8
SLOTS = 10
EARLY = 4
PARTS = 1
PIECES = 1
STAGES = 8
MESH = pl.DeviceIdType.MESH
F32, BF16 = jnp.float32, jnp.bfloat16

epsilon = 1e-06


def divisor(size, most):
    return max(k for k in range(128, most + 1, 128) if size % k == 0)


def placement(routed, ranks, capacity, groups, count):
    row = lax.broadcasted_iota(jnp.int32, (count * capacity, routed.shape[1]), 0)
    owner = row // (capacity * groups)
    return jnp.where((owner == routed) & (row % capacity == ranks), 1.0, 0.0).astype(F32)


def kernel(
    sections, n, capacity, act_hbm, gain_hbm, ids_hbm, first_hbm, second_hbm, out,
    act, gain, ids, pool, normed, packed, received, total, hidden, outgoing, returned,
    where_to, residual, where_from,
    small_sem, pool_sem, pass_send, pass_recv, send_sem, recv_sem, back_send, back_recv, stage_sem,
):
    section, me = lax.axis_index("section"), lax.axis_index("expert")
    following = lax.rem(section + 1, sections)
    groups = n // EXPERTS
    tokens, width = act.shape
    ff = hidden.shape[1]
    steps, depth = packed.shape[0], packed.shape[3]
    sends, piece_columns = outgoing.shape[0], outgoing.shape[3]
    columns = pool.shape[2]
    slots = pool.shape[0]
    chunks = tiles = width // columns
    loads = chunks + tiles
    block = math.gcd(ff, columns)
    across = columns // block

    def place(j):
        return (j // across) * columns, (j % across) * block

    def load_first(c):
        rows = pl.ds(pl.multiple_of(c * columns, columns), columns)
        for j in range(ff // block):
            top, left = place(j)
            pltpu.make_async_copy(
                first_hbm.at[0, rows, j * block:(j + 1) * block],
                pool.at[c, top:top + columns, left:left + block],
                pool_sem.at[c],
            ).start()

    def wait_first(c):
        rows = first_hbm.at[0, pl.ds(pl.multiple_of(c * columns, columns), columns), :]
        pltpu.make_async_copy(rows, rows, pool_sem.at[c]).wait()

    def second_copy(t):
        cols = pl.ds(pl.multiple_of(t * columns, columns), columns)
        slot = lax.rem(t + chunks, slots)
        return pltpu.make_async_copy(second_hbm.at[0, :, cols], pool.at[slot, 0:ff, :], pool_sem.at[slot])

    def dispatch(c, peer):
        pltpu.make_async_remote_copy(
            src_ref=packed.at[c, peer // groups],
            dst_ref=received.at[c, me],
            send_sem=send_sem.at[c],
            recv_sem=recv_sem.at[c],
            device_id=(section, peer),
            device_id_type=MESH,
        ).start()

    smalls = [
        pltpu.make_async_copy(act_hbm.at[0], act, small_sem.at[0]),
        pltpu.make_async_copy(gain_hbm, gain, small_sem.at[1]),
        pltpu.make_async_copy(ids_hbm, ids, small_sem.at[2]),
    ]
    line = n // 2
    staged = n % 2 == 0 and line <= STAGES
    at = me // 2
    pair = me + 1 - 2 * lax.rem(me, 2)

    def ahead(distance, act_on):
        for base, by in ((me, distance), (pair, distance - 1)):
            if by == 0:
                act_on(base)
            elif by < line:
                @pl.when(at + by < line)
                def _():
                    act_on(base + 2 * by)

                @pl.when(at >= by)
                def _():
                    act_on(base - 2 * by)

    reach = (line + 1) // 2
    near_count = 1
    for by in range(1, reach + 1):
        both = 1 if by == reach else 2
        near_count += both * (jnp.where(at >= by, 1, 0) + jnp.where(at + by < line, 1, 0))

    def near(act_on):
        for distance in range(1, reach + 1):
            ahead(distance, act_on)

    def greet(sem, peer_section, peer):
        pl.semaphore_signal(sem, inc=1, device_id=(peer_section, peer), device_id_type=MESH)

    barrier = pltpu.get_barrier_semaphore()
    previous = lax.rem(section + sections - 1, sections)
    for copy in smalls:
        copy.start()
    if staged:
        near(lambda peer: greet(barrier, section, peer))
        greet(barrier, previous, me)
    else:
        def greet_one(i, carry):
            greet(barrier, section, lax.rem(me + i, n))
            return carry

        def greet_previous(i, carry):
            greet(barrier, previous, i)
            return carry

        lax.fori_loop(1, n, greet_one, 0)
        lax.fori_loop(0, n, greet_previous, 0)

    def start_first(c, carry):
        load_first(c)
        return carry

    def start_second(t, carry):
        second_copy(t).start()
        return carry

    lax.fori_loop(0, chunks, start_first, 0)
    lax.fori_loop(0, slots - chunks, start_second, 0)

    for copy in smalls:
        copy.wait()
    floats = act[...].astype(F32)
    scale = lax.rsqrt(jnp.mean(floats * floats, axis=-1, keepdims=True) + epsilon)
    normed[...] = (floats * scale * gain[...]).astype(BF16)
    routed = ids[...]
    expert = lax.broadcasted_iota(jnp.int32, (EXPERTS, tokens), 0)
    onehot = jnp.where(expert == routed, 1.0, 0.0).astype(F32)
    earlier = lax.broadcasted_iota(jnp.int32, (tokens, tokens), 0) < lax.broadcasted_iota(
        jnp.int32, (tokens, tokens), 1
    )
    before = jnp.dot(
        onehot.astype(BF16), jnp.where(earlier, 1.0, 0.0).astype(BF16), preferred_element_type=F32
    )
    ranks = jnp.sum(before * onehot, axis=0, keepdims=True).astype(jnp.int32)
    placing = placement(routed, ranks, capacity, 1, EXPERTS).astype(BF16)
    for c in range(steps):
        rows = jnp.dot(placing, normed[:, c * depth:(c + 1) * depth], preferred_element_type=F32)
        packed[c] = rows.astype(BF16).reshape(EXPERTS, capacity, depth)
    back = placement(routed, ranks, capacity, groups, where_to.shape[1] // capacity)
    where_to[...] = back.T.astype(BF16)

    def over_steps(low, high, *distances):
        def one(c, carry):
            for distance in distances:
                ahead(distance, lambda peer: dispatch(c, peer))
            return carry

        lax.fori_loop(low, high, one, 0)

    passes = [
        pltpu.make_async_remote_copy(
            src_ref=src, dst_ref=dst, send_sem=pass_send.at[k], recv_sem=pass_recv.at[k],
            device_id=(following, me), device_id_type=MESH,
        )
        for k, (src, dst) in enumerate(((act, residual), (where_to, where_from)))
    ]
    half = n // 2
    if staged:
        early = min(steps, EARLY)
        pl.semaphore_wait(barrier, near_count + 1)
        near(lambda peer: greet(stage_sem, section, peer))
        close, farther = tuple(range(reach, 0, -1)), tuple(range(line, reach, -1))
        over_steps(0, early, *close)
        pl.semaphore_wait(stage_sem, near_count)
        over_steps(0, early, *farther)
        over_steps(early, steps, *farther, *close)
        for copy in passes:
            copy.start()
    else:
        pl.semaphore_wait(barrier, 2 * n - 1)

        def one(c, carry):
            def to_one(i, inner):
                step = (i + 1) // 2
                dispatch(c, lax.rem(me + half + jnp.where(lax.rem(i, 2) == 0, step, n - step), n))
                return inner

            lax.fori_loop(0, n - 1, to_one, 0)
            return carry

        lax.fori_loop(0, steps, one, 0)
        for copy in passes:
            copy.start()

    def keep(c, carry):
        pltpu.make_async_copy(packed.at[c, me // groups], received.at[c, me], recv_sem.at[c]).start()
        return carry

    lax.fori_loop(0, steps, keep, 0)

    parts = steps // chunks

    def multiply(c, kind):
        wait_first(c)
        for p in range(parts):
            step = c * parts + p
            pltpu.make_async_copy(received.at[step], received.at[step], recv_sem.at[step]).wait()
            rows = received[step].reshape(n * capacity, depth)
            for j in range(ff // block):
                top, left = place(j)
                cols = slice(j * block, (j + 1) * block)
                value = jnp.dot(
                    rows, pool[c, top + p * depth:top + (p + 1) * depth, left:left + block],
                    preferred_element_type=F32,
                )
                if kind != "start" or p:
                    value = value + total[:, cols]
                if kind == "end" and p == parts - 1:
                    hidden[:, cols] = jax.nn.gelu(value, approximate=True).astype(BF16)
                else:
                    total[:, cols] = value

    def more(c):
        @pl.when(c + slots < loads)
        def _():
            second_copy(c + slots - chunks).start()

    multiply(0, "start")
    more(0)

    def middle(c, carry):
        multiply(c, "middle")
        more(c)
        return carry

    lax.fori_loop(1, chunks - 1, middle, 0)
    multiply(chunks - 1, "end")
    more(chunks - 1)

    pieces = sends // tiles

    def tile(t, carry):
        second_copy(t).wait()
        slot = lax.rem(t + chunks, slots)
        for j in range(pieces):
            cols = slice(j * piece_columns, (j + 1) * piece_columns)
            piece = jnp.dot(hidden[...], pool[slot, 0:ff, cols], preferred_element_type=F32)
            u = t * pieces + j
            outgoing[u] = piece.astype(BF16).reshape(n, capacity, piece_columns)

            def give(i, inner):
                peer = lax.rem(half * (1 - me // half + i // half) + lax.rem(me + i, half), n)
                pltpu.make_async_remote_copy(
                    src_ref=outgoing.at[u, peer],
                    dst_ref=returned.at[u, me],
                    send_sem=back_send.at[u],
                    recv_sem=back_recv.at[u],
                    device_id=(following, peer),
                    device_id_type=MESH,
                ).start()
                return inner

            lax.fori_loop(0, n, give, 0)
        @pl.when(t + chunks + slots < loads)
        def _():
            second_copy(t + slots).start()

        return carry

    lax.fori_loop(0, tiles, tile, 0)

    for copy in passes:
        copy.wait()
    picks = where_from[:, :n * capacity]

    def combine(u, carry):
        pltpu.make_async_copy(returned.at[u], returned.at[u], back_recv.at[u]).wait()
        cols = pl.ds(pl.multiple_of(u * piece_columns, piece_columns), piece_columns)
        mixed = jnp.dot(picks, returned[u].reshape(n * capacity, piece_columns), preferred_element_type=F32)
        out[0, :, cols] = (residual[:, cols].astype(F32) + mixed).astype(BF16)
        return carry

    lax.fori_loop(0, sends, combine, 0)

    def finish(u, carry):
        pltpu.make_async_copy(outgoing.at[u], outgoing.at[u], back_send.at[u]).wait()
        return carry

    lax.fori_loop(0, sends, finish, 0)

    def drain(c, carry):
        done = received.at[c, pl.ds(0, n - 1)]
        pltpu.make_async_copy(done, done, send_sem.at[c]).wait()
        return carry

    lax.fori_loop(0, steps, drain, 0)


def per_device(sections, n, activations, norm_gain, in_proj, out_proj, expert_ids):
    tokens, width = activations.shape[1:]
    ff = in_proj.shape[2]
    capacity = 2 * tokens // EXPERTS
    columns = divisor(width, 512)
    depth, piece_columns = columns // PARTS, columns // PIECES
    chunks = width // columns
    steps, sends = width // depth, width // piece_columns
    slots = max(chunks, min(SLOTS, 2 * chunks))
    block = math.gcd(ff, columns)
    bands = -(-(ff // block) // (columns // block))
    rows = n * capacity
    lanes = max(128, rows)
    dma = pltpu.SemaphoreType.DMA
    return pl.pallas_call(
        functools.partial(kernel, sections, n, capacity),
        out_shape=pltpu.VMEM(activations.shape, activations.dtype),
        in_specs=[pl.BlockSpec(memory_space=pl.ANY)] * 5,
        out_specs=pl.BlockSpec(memory_space=pltpu.VMEM),
        scratch_shapes=[
            pltpu.VMEM((tokens, width), BF16),
            pltpu.VMEM((1, width), F32),
            pltpu.VMEM((1, tokens), jnp.int32),
            pltpu.VMEM((slots, max(ff, bands * columns), columns), BF16),
            pltpu.VMEM((tokens, width), BF16),
            pltpu.VMEM((steps, EXPERTS, capacity, depth), BF16),
            pltpu.VMEM((steps, n, capacity, depth), BF16),
            pltpu.VMEM((rows, ff), F32),
            pltpu.VMEM((rows, ff), BF16),
            pltpu.VMEM((sends, n, capacity, piece_columns), BF16),
            pltpu.VMEM((sends, n, capacity, piece_columns), BF16),
            pltpu.VMEM((tokens, lanes), BF16),
            pltpu.VMEM((tokens, width), BF16),
            pltpu.VMEM((tokens, lanes), BF16),
            dma((3,)),
            dma((slots,)),
            dma((2,)),
            dma((2,)),
            dma((steps,)),
            dma((steps,)),
            dma((sends,)),
            dma((sends,)),
            pltpu.SemaphoreType.REGULAR,
        ],
        compiler_params=pltpu.CompilerParams(
            collective_id=0, has_side_effects=True, vmem_limit_bytes=62 * 1024 * 1024
        ),
    )(activations, norm_gain, expert_ids.reshape(1, tokens), in_proj, out_proj)


def solution(mesh):
    return jax.shard_map(
        functools.partial(per_device, mesh.shape["section"], mesh.shape["expert"]),
        mesh=mesh,
        in_specs=(
            P("section", "expert", None),
            P("section", None),
            P("section", None, "expert"),
            P("section", "expert", None),
            P("section", "expert", None),
        ),
        out_specs=P("section", "expert", None),
        check_vma=False,
    )
```

```python
import functools
import math

import jax
import jax.numpy as jnp
from jax import lax
from jax.experimental import pallas as pl
from jax.experimental.pallas import tpu as pltpu
from jax.sharding import PartitionSpec as P

EXPERTS = 8
SLOTS = 10
PARTS = 1
PIECES = 1
MESH = pl.DeviceIdType.MESH
F32, BF16 = jnp.float32, jnp.bfloat16

epsilon = 1e-06


def divisor(size, most):
    return max(k for k in range(128, most + 1, 128) if size % k == 0)


def placement(routed, ranks, capacity, groups, count):
    row = lax.broadcasted_iota(jnp.int32, (count * capacity, routed.shape[1]), 0)
    owner = row // (capacity * groups)
    return jnp.where((owner == routed) & (row % capacity == ranks), 1.0, 0.0).astype(F32)


def kernel(
    sections, n, capacity, act_hbm, gain_hbm, ids_hbm, first_hbm, second_hbm, out,
    act, gain, ids, pool, normed, packed, received, total, hidden, outgoing, returned,
    where_to, residual, where_from,
    small_sem, pool_sem, pass_send, pass_recv, send_sem, recv_sem, back_send, back_recv,
):
    section, me = lax.axis_index("section"), lax.axis_index("expert")
    following = lax.rem(section + 1, sections)
    groups = n // EXPERTS
    tokens, width = act.shape
    ff = hidden.shape[1]
    steps, depth = packed.shape[0], packed.shape[3]
    sends, piece_columns = outgoing.shape[0], outgoing.shape[3]
    columns = pool.shape[2]
    slots = pool.shape[0]
    chunks = tiles = width // columns
    loads = chunks + tiles
    block = math.gcd(ff, columns)
    across = columns // block

    def place(j):
        return (j // across) * columns, (j % across) * block

    def load_first(c):
        rows = pl.ds(pl.multiple_of(c * columns, columns), columns)
        for j in range(ff // block):
            top, left = place(j)
            pltpu.make_async_copy(
                first_hbm.at[0, rows, j * block:(j + 1) * block],
                pool.at[c, top:top + columns, left:left + block],
                pool_sem.at[c],
            ).start()

    def wait_first(c):
        rows = first_hbm.at[0, pl.ds(pl.multiple_of(c * columns, columns), columns), :]
        pltpu.make_async_copy(rows, rows, pool_sem.at[c]).wait()

    def second_copy(t):
        cols = pl.ds(pl.multiple_of(t * columns, columns), columns)
        slot = lax.rem(t + chunks, slots)
        return pltpu.make_async_copy(second_hbm.at[0, :, cols], pool.at[slot, 0:ff, :], pool_sem.at[slot])

    def dispatch(c, peer):
        pltpu.make_async_remote_copy(
            src_ref=packed.at[c, peer // groups],
            dst_ref=received.at[c, me],
            send_sem=send_sem.at[c],
            recv_sem=recv_sem.at[c],
            device_id=(section, peer),
            device_id_type=MESH,
        ).start()

    smalls = [
        pltpu.make_async_copy(act_hbm.at[0], act, small_sem.at[0]),
        pltpu.make_async_copy(gain_hbm, gain, small_sem.at[1]),
        pltpu.make_async_copy(ids_hbm, ids, small_sem.at[2]),
    ]

    def greet(sem, peer_section, peer):
        pl.semaphore_signal(sem, inc=1, device_id=(peer_section, peer), device_id_type=MESH)

    barrier = pltpu.get_barrier_semaphore()
    previous = lax.rem(section + sections - 1, sections)
    for copy in smalls:
        copy.start()
    def greet_one(i, carry):
        greet(barrier, section, lax.rem(me + i, n))
        return carry

    def greet_previous(i, carry):
        greet(barrier, previous, i)
        return carry

    lax.fori_loop(1, n, greet_one, 0)
    lax.fori_loop(0, n, greet_previous, 0)

    def start_first(c, carry):
        load_first(c)
        return carry

    def start_second(t, carry):
        second_copy(t).start()
        return carry

    lax.fori_loop(0, chunks, start_first, 0)
    lax.fori_loop(0, slots - chunks, start_second, 0)

    for copy in smalls:
        copy.wait()
    floats = act[...].astype(F32)
    scale = lax.rsqrt(jnp.mean(floats * floats, axis=-1, keepdims=True) + epsilon)
    normed[...] = (floats * scale * gain[...]).astype(BF16)
    routed = ids[...]
    expert = lax.broadcasted_iota(jnp.int32, (EXPERTS, tokens), 0)
    onehot = jnp.where(expert == routed, 1.0, 0.0).astype(F32)
    earlier = lax.broadcasted_iota(jnp.int32, (tokens, tokens), 0) < lax.broadcasted_iota(
        jnp.int32, (tokens, tokens), 1
    )
    before = jnp.dot(
        onehot.astype(BF16), jnp.where(earlier, 1.0, 0.0).astype(BF16), preferred_element_type=F32
    )
    ranks = jnp.sum(before * onehot, axis=0, keepdims=True).astype(jnp.int32)
    placing = placement(routed, ranks, capacity, 1, EXPERTS).astype(BF16)
    for c in range(steps):
        rows = jnp.dot(placing, normed[:, c * depth:(c + 1) * depth], preferred_element_type=F32)
        packed[c] = rows.astype(BF16).reshape(EXPERTS, capacity, depth)
    back = placement(routed, ranks, capacity, groups, where_to.shape[1] // capacity)
    where_to[...] = back.T.astype(BF16)

    passes = [
        pltpu.make_async_remote_copy(
            src_ref=src, dst_ref=dst, send_sem=pass_send.at[k], recv_sem=pass_recv.at[k],
            device_id=(following, me), device_id_type=MESH,
        )
        for k, (src, dst) in enumerate(((act, residual), (where_to, where_from)))
    ]
    half = n // 2
    pl.semaphore_wait(barrier, 2 * n - 1)

    def one(c, carry):
        def to_one(i, inner):
            dispatch(c, lax.rem(half * (1 - me // half + i // half) + lax.rem(me + i + i // half, half), n))
            return inner

        lax.fori_loop(0, n - 1, to_one, 0)
        return carry

    lax.fori_loop(0, steps, one, 0)
    for copy in passes:
        copy.start()

    def keep(c, carry):
        pltpu.make_async_copy(packed.at[c, me // groups], received.at[c, me], recv_sem.at[c]).start()
        return carry

    lax.fori_loop(0, steps, keep, 0)

    parts = steps // chunks

    def multiply(c, kind):
        wait_first(c)
        for p in range(parts):
            step = c * parts + p
            pltpu.make_async_copy(received.at[step], received.at[step], recv_sem.at[step]).wait()
            rows = received[step].reshape(n * capacity, depth)
            for j in range(ff // block):
                top, left = place(j)
                cols = slice(j * block, (j + 1) * block)
                value = jnp.dot(
                    rows, pool[c, top + p * depth:top + (p + 1) * depth, left:left + block],
                    preferred_element_type=F32,
                )
                if kind != "start" or p:
                    value = value + total[:, cols]
                if kind == "end" and p == parts - 1:
                    hidden[:, cols] = jax.nn.gelu(value, approximate=True).astype(BF16)
                else:
                    total[:, cols] = value

    def more(c):
        @pl.when(c + slots < loads)
        def _():
            second_copy(c + slots - chunks).start()

    multiply(0, "start")
    more(0)

    def middle(c, carry):
        multiply(c, "middle")
        more(c)
        return carry

    lax.fori_loop(1, chunks - 1, middle, 0)
    second_copy(0).wait()
    multiply(chunks - 1, "end")
    more(chunks - 1)

    pieces = sends // tiles

    def tile(t, carry):
        if not isinstance(t, int):
            second_copy(t).wait()
        slot = lax.rem(t + chunks, slots)
        for j in range(pieces):
            cols = slice(j * piece_columns, (j + 1) * piece_columns)
            piece = jnp.dot(hidden[...], pool[slot, 0:ff, cols], preferred_element_type=F32)
            u = t * pieces + j
            outgoing[u] = piece.astype(BF16).reshape(n, capacity, piece_columns)

            def give(i, inner):
                peer = lax.rem(half * (1 - me // half + i // half) + lax.rem(me + i, half), n)
                pltpu.make_async_remote_copy(
                    src_ref=outgoing.at[u, peer],
                    dst_ref=returned.at[u, me],
                    send_sem=back_send.at[u],
                    recv_sem=back_recv.at[u],
                    device_id=(following, peer),
                    device_id_type=MESH,
                ).start()
                return inner

            lax.fori_loop(0, n, give, 0)
        @pl.when(t + chunks + slots < loads)
        def _():
            second_copy(t + slots).start()

        return carry

    tile(0, 0)
    lax.fori_loop(1, tiles, tile, 0)

    for copy in passes:
        copy.wait()
    picks = where_from[:, :n * capacity]

    def combine(u, carry):
        pltpu.make_async_copy(returned.at[u], returned.at[u], back_recv.at[u]).wait()
        cols = pl.ds(pl.multiple_of(u * piece_columns, piece_columns), piece_columns)
        mixed = jnp.dot(picks, returned[u].reshape(n * capacity, piece_columns), preferred_element_type=F32)
        out[0, :, cols] = (residual[:, cols].astype(F32) + mixed).astype(BF16)
        return carry

    lax.fori_loop(0, sends, combine, 0)

    def finish(u, carry):
        pltpu.make_async_copy(outgoing.at[u], outgoing.at[u], back_send.at[u]).wait()
        return carry

    lax.fori_loop(0, sends, finish, 0)

    def drain(c, carry):
        done = received.at[c, pl.ds(0, n - 1)]
        pltpu.make_async_copy(done, done, send_sem.at[c]).wait()
        return carry

    lax.fori_loop(0, steps, drain, 0)


def per_device(sections, n, activations, norm_gain, in_proj, out_proj, expert_ids):
    tokens, width = activations.shape[1:]
    ff = in_proj.shape[2]
    capacity = 2 * tokens // EXPERTS
    columns = divisor(width, 512)
    depth, piece_columns = columns // PARTS, columns // PIECES
    chunks = width // columns
    steps, sends = width // depth, width // piece_columns
    slots = max(chunks, min(SLOTS, 2 * chunks))
    block = math.gcd(ff, columns)
    bands = -(-(ff // block) // (columns // block))
    rows = n * capacity
    lanes = max(128, rows)
    dma = pltpu.SemaphoreType.DMA
    return pl.pallas_call(
        functools.partial(kernel, sections, n, capacity),
        out_shape=pltpu.VMEM(activations.shape, activations.dtype),
        in_specs=[pl.BlockSpec(memory_space=pl.ANY)] * 5,
        out_specs=pl.BlockSpec(memory_space=pltpu.VMEM),
        scratch_shapes=[
            pltpu.VMEM((tokens, width), BF16),
            pltpu.VMEM((1, width), F32),
            pltpu.VMEM((1, tokens), jnp.int32),
            pltpu.VMEM((slots, max(ff, bands * columns), columns), BF16),
            pltpu.VMEM((tokens, width), BF16),
            pltpu.VMEM((steps, EXPERTS, capacity, depth), BF16),
            pltpu.VMEM((steps, n, capacity, depth), BF16),
            pltpu.VMEM((rows, ff), F32),
            pltpu.VMEM((rows, ff), BF16),
            pltpu.VMEM((sends, n, capacity, piece_columns), BF16),
            pltpu.VMEM((sends, n, capacity, piece_columns), BF16),
            pltpu.VMEM((tokens, lanes), BF16),
            pltpu.VMEM((tokens, width), BF16),
            pltpu.VMEM((tokens, lanes), BF16),
            dma((3,)),
            dma((slots,)),
            dma((2,)),
            dma((2,)),
            dma((steps,)),
            dma((steps,)),
            dma((sends,)),
            dma((sends,)),
        ],
        compiler_params=pltpu.CompilerParams(
            collective_id=0, has_side_effects=True, vmem_limit_bytes=62 * 1024 * 1024
        ),
    )(activations, norm_gain, expert_ids.reshape(1, tokens), in_proj, out_proj)


def solution(mesh):
    return jax.shard_map(
        functools.partial(per_device, mesh.shape["section"], mesh.shape["expert"]),
        mesh=mesh,
        in_specs=(
            P("section", "expert", None),
            P("section", None),
            P("section", None, "expert"),
            P("section", "expert", None),
            P("section", "expert", None),
        ),
        out_specs=P("section", "expert", None),
        check_vma=False,
    )
```
